32 devices in a mesh: gx: 4 (over y, x), gy: 8 (over z, core).
Axes of the slice: x: 2, y: 2, z: 4, core: 2. Of those that a mesh axis runs over, the one named last changes fastest.
Arguments:
- expert_grad: bfloat16 [8, 512, 14336], P('gx', None, 'gy'), may hold values from -40000 to 40000
- attn_grad: bfloat16 [4, 2048, 4096], P('gx', None, 'gy'), may hold values from -40000 to 40000
- expert_master: float32 [4096, 14336], P(('gx', 'gy')), may hold values from -0.75 to 0.75
- expert_moment: float32 [4096, 14336], P(('gx', 'gy')), may hold values from -6 to 6
- expert_second: float32 [4096, 14336], P(('gx', 'gy')), may hold values from 0.1 to 4
- attn_master: float32 [2048, 4096], P(('gx', 'gy')), may hold values from -0.75 to 0.75
- attn_moment: float32 [2048, 4096], P(('gx', 'gy')), may hold values from -6 to 6
- attn_second: float32 [2048, 4096], P(('gx', 'gy')), may hold values from 0.1 to 4
Outputs:
- expert_master_new: float32 [4096, 14336], P(('gx', 'gy'))
- expert_moment_new: float32 [4096, 14336], P(('gx', 'gy'))
- expert_second_new: float32 [4096, 14336], P(('gx', 'gy'))
- attn_master_new: float32 [2048, 4096], P(('gx', 'gy'))
- attn_moment_new: float32 [2048, 4096], P(('gx', 'gy'))
- attn_second_new: float32 [2048, 4096], P(('gx', 'gy'))
- expert_weight: bfloat16 [8, 512, 14336], P('gx', None, 'gy')
- attn_weight: bfloat16 [2048, 4096], P(None, 'gy')
The draws below stay inside these ranges and needn't reach their ends.
All inputs are finite; a program needn't handle non-finite values.
Results may differ from the reference program's by a relative error of at most 0.001.
Values may be sent and summed in bfloat16 or wider, within the bound.
A program may use at most 128 MiB of HBM per device.

```python
import math
import jax
import jax.numpy as jnp
from jax import lax

E = 8
FF = 14336
QW = 4096
EROWS = 512
AROWS = 2048
REPLICAS = 4
NUMEL = 67108864


def draw_expert_grad(key, part):
    keys = jax.random.split(key, 3)
    row_scale = jnp.exp(jax.random.uniform(keys[1], (E, EROWS, 1), jnp.float32) * jnp.log(10.0))
    col_scale = jnp.exp(jax.random.uniform(keys[2], (1, 1, FF), jnp.float32) * jnp.log(10.0))
    position = jnp.arange(E * EROWS, dtype=jnp.float32).reshape(E, EROWS, 1) / (E * EROWS - 1)
    ramp = 10.0 ** position
    base = jnp.clip(jax.random.normal(keys[0], (E, EROWS, FF), jnp.float32), -6.0, 6.0)
    return (base * row_scale * col_scale * ramp).astype(jnp.bfloat16)


def draw_attn_grad(key, part):
    keys = jax.random.split(key, 3)
    row_scale = jnp.exp(jax.random.uniform(keys[1], (1, AROWS, 1), jnp.float32) * jnp.log(10.0))
    col_scale = jnp.exp(jax.random.uniform(keys[2], (1, 1, QW), jnp.float32) * jnp.log(10.0))
    replica_ramp = (2.0 ** (jnp.arange(REPLICAS, dtype=jnp.float32) / (REPLICAS - 1)))[:, None, None]
    position = (jnp.arange(AROWS, dtype=jnp.float32) / (AROWS - 1))[None, :, None]
    ramp = replica_ramp * 10.0 ** position
    base = jnp.clip(jax.random.normal(keys[0], (REPLICAS, AROWS, QW), jnp.float32), -6.0, 6.0)
    return (base * row_scale * col_scale * ramp).astype(jnp.bfloat16)


def shard_levels(stream_key, shape, shards, least, high):
    def one(axis_at, blocks):
        heights = jax.random.uniform(jax.random.fold_in(jax.random.fold_in(stream_key, 6), axis_at), (blocks,), jnp.float32, least / len(shards), high / len(shards))
        return jnp.repeat(jnp.exp(heights), shape[axis_at] // blocks).reshape((-1,) + (1,) * (len(shape) - axis_at - 1))

    factor_of = one(*shards[0])
    for cut in shards[1:]:
        factor_of = factor_of * one(*cut)
    return factor_of


def noise(rng, shape, width, most, cuts=(), held_as=jnp.bfloat16):
    factor_of = shard_levels(rng, shape, cuts, -0.22, 0.18) if cuts else 1.0
    values = jax.random.normal(rng, shape, jnp.float32) * width * factor_of
    return jnp.minimum(jnp.maximum(values, -most), most).astype(held_as)


def setup_inputs(seed: int = 0) -> dict:
    key_list = jax.random.split(jax.random.key(seed), 9)
    expert_grad = draw_expert_grad(jax.random.fold_in(key_list[8], 71), 0)
    attn_grad = draw_attn_grad(jax.random.fold_in(key_list[8], 71), 0)
    expert_master = noise(key_list[2], (E * EROWS, FF), 0.05, 0.75, ((0, 32),), jnp.float32)
    expert_moment = noise(key_list[3], (E * EROWS, FF), 1.0, 6.0, ((0, 32),), jnp.float32)
    expert_second = jnp.clip(jnp.exp(math.log(4.0) - 3.6888794 * jax.random.uniform(key_list[4], (E * EROWS, FF), jnp.float32) ** shard_levels(key_list[4], (E * EROWS, FF), ((0, 32),), -0.2, 0.2)), 0.1, 4.0)
    attn_master = noise(key_list[5], (AROWS, QW), 0.05, 0.75, ((0, 32),), jnp.float32)
    attn_moment = noise(key_list[6], (AROWS, QW), 1.0, 6.0, ((0, 32),), jnp.float32)
    attn_second = jnp.clip(jnp.exp(math.log(4.0) - 3.6888794 * jax.random.uniform(key_list[7], (AROWS, QW), jnp.float32) ** shard_levels(key_list[7], (AROWS, QW), ((0, 32),), -0.2, 0.2)), 0.1, 4.0)
    return {"expert_grad": expert_grad, "attn_grad": attn_grad, "expert_master": expert_master, "expert_moment": expert_moment, "expert_second": expert_second, "attn_master": attn_master, "attn_moment": attn_moment, "attn_second": attn_second}


beta_one = 0.9
beta_two = 0.95
learn_rate = 0.01
weight_decay = 0.1
adam_eps = 1e-08
bias_one = 1.0 - 0.9 ** 20
bias_two = 1.0 - 0.95 ** 20

def adam_update(gradient, master, moment, second, clip_factor):
    scaled = clip_factor * gradient
    moment_new = beta_one * moment + (1.0 - beta_one) * scaled
    second_new = beta_two * second + (1.0 - beta_two) * scaled * scaled
    update = moment_new / bias_one / (jnp.sqrt(second_new / bias_two) + adam_eps)
    master_new = master - learn_rate * (update + weight_decay * master)
    return (master_new, moment_new, second_new)

def reference(expert_grad, attn_grad, expert_master, expert_moment, expert_second, attn_master, attn_moment, attn_second):
    expert_flat = expert_grad.astype(jnp.float32).reshape(E * EROWS, FF)
    attn_sum = lax.optimization_barrier(jnp.sum(attn_grad.astype(jnp.float32), axis=0))
    total = jnp.sum(expert_flat * expert_flat) + jnp.sum(attn_sum * attn_sum)
    clip_factor = 1.0 / jnp.sqrt(total / NUMEL + 1e-06)
    e_master, e_moment, e_second = adam_update(expert_flat, expert_master, expert_moment, expert_second, clip_factor)
    a_master, a_moment, a_second = adam_update(attn_sum, attn_master, attn_moment, attn_second, clip_factor)
    expert_weight = e_master.astype(jnp.bfloat16).reshape(E, EROWS, FF)
    attn_weight = a_master.astype(jnp.bfloat16)
    return (e_master, e_moment, e_second, a_master, a_moment, a_second, expert_weight, attn_weight)
```

```python
import functools
import math

import jax
import jax.numpy as jnp
from jax import lax
from jax.experimental import pallas as pl
from jax.experimental.pallas import tpu as pltpu
from jax.sharding import PartitionSpec as P

MESH = pl.DeviceIdType.MESH

beta_one = 0.9
beta_two = 0.95
learn_rate = 0.01
weight_decay = 0.1
adam_eps = 1e-08
bias_one = 1.0 - 0.9**20
bias_two = 1.0 - 0.95**20


def adam_update(gradient, master, moment, second, clip_factor):
    scaled = clip_factor * gradient
    moment_new = beta_one * moment + (1.0 - beta_one) * scaled
    second_new = beta_two * second + (1.0 - beta_two) * scaled * scaled
    update = moment_new / bias_one / (jnp.sqrt(second_new / bias_two) + adam_eps)
    master_new = master - learn_rate * (update + weight_decay * master)
    return (master_new, moment_new, second_new)


def partner_to(me, k, n):
    if n & (n - 1):
        return lax.rem(me + k, n)
    out, bit = me, 1
    while bit < n:
        if k & bit:
            out = out + bit * (1 - 2 * lax.rem(me // bit, 2))
        bit *= 2
    return out


def partner_from(me, k, n):
    if n & (n - 1):
        return lax.rem(me + n - k, n)
    return partner_to(me, k, n)


def send_order(n):
    return list(range(n - 1, 0, -1))


def col_chunk(width):
    return 256 if width % 256 == 0 else 128


def row_chunk(rows):
    return math.gcd(rows, 16)


top = 2.0**15.5
floor = 2.0**-15.5


def encode(x):
    square = x * x
    fourth = square * square
    eighth = jnp.where(jnp.abs(x) < floor, 0.0, fourth * fourth)
    return jnp.where(x < 0.0, -eighth, eighth)


def decode(y):
    root = jnp.sqrt(jnp.sqrt(jnp.sqrt(jnp.abs(y))))
    return jnp.where(y < 0.0, -root, root)


def step_kernel(
    n_out, n_in, numel,
    eg, ag, em, eo, es, am, ao, as_,
    em_o, eo_o, es_o, am_o, ao_o, as_o, ew_o, aw_o,
    mine, held, arep, asum, acode, agot, part, acc,
    own_sem, state_sem, f_send, f_recv, g_send, g_recv, h_send, h_recv,
    p_send, p_recv, q_send, q_recv, r_send, r_recv, s_send, s_recv, t_send, t_recv,
):
    out_me = lax.axis_index("gx")
    in_me = lax.axis_index("gy")
    rows, width = held.shape[1], held.shape[2]
    block_rows, a_width = arep.shape[1], arep.shape[2]
    a_rows = agot.shape[1]

    def to_in(k):
        return (out_me, partner_to(in_me, k, n_in))

    def to_out(k):
        return (partner_to(out_me, k, n_out), in_me)

    def remote(src, dst, send, recv, where):
        return pltpu.make_async_remote_copy(
            src_ref=src, dst_ref=dst, send_sem=send, recv_sem=recv,
            device_id=where, device_id_type=MESH,
        )

    def rows_at(ref, index, count):
        return ref.at[pl.ds(pl.multiple_of(index * count, count), count)]

    barrier = pltpu.get_barrier_semaphore()
    for k in range(1, n_in):
        pl.semaphore_signal(barrier, inc=1, device_id=to_in(k), device_id_type=MESH)
    for k in range(1, n_out):
        pl.semaphore_signal(barrier, inc=1, device_id=to_out(k), device_id_type=MESH)

    load_grad = pltpu.make_async_copy(eg, mine, own_sem.at[0])
    load_grad.start()
    load_rep = pltpu.make_async_copy(rows_at(ag, out_me, block_rows), arep.at[0], own_sem.at[1])
    load_rep.start()
    pl.semaphore_wait(barrier, n_in - 1 + n_out - 1)

    rep_copies = {}
    for k in send_order(n_out):
        c = remote(
            rows_at(ag, partner_to(out_me, k, n_out), block_rows), arep.at[k],
            g_send.at[k], g_recv.at[k], to_out(k),
        )
        c.start()
        rep_copies[k] = c
    order = send_order(n_in)
    far, near = order[: n_in // 2], order[n_in // 2 :]
    first = far[: n_in // 4] + near[:1]
    rest = near[1:] + far[n_in // 4 :]
    arrival = first + near[1:] + [0] + far[n_in // 4 :]
    fwd = {}

    def send_fwd(k):
        c = remote(
            rows_at(eg, partner_to(in_me, k, n_in), rows), held.at[k],
            f_send.at[k], f_recv.at[k], to_in(k),
        )
        c.start()
        fwd[k] = c

    for k in first:
        send_fwd(k)

    state = []
    for i, (src, dst) in enumerate(
        ((em, em_o), (eo, eo_o), (es, es_o), (am, am_o), (ao, ao_o), (as_, as_o))
    ):
        c = pltpu.make_async_copy(src, dst, state_sem.at[i])
        c.start()
        state.append(c)

    load_grad.wait()
    chunk = col_chunk(width)
    rc = row_chunk(mine.shape[0])

    def square_rows(i, carry):
        r = pl.ds(pl.multiple_of(i * rc, rc), rc)
        for c in range(width // chunk):
            x = mine[r, c * chunk : (c + 1) * chunk].astype(jnp.float32)
            carry = carry + x * x
        return carry

    e_sq = lax.fori_loop(0, mine.shape[0] // rc, square_rows, jnp.zeros((rc, chunk), jnp.float32))

    load_rep.wait()
    for k in send_order(n_out):
        rep_copies[k].wait_recv()
    a_chunk = col_chunk(a_width)
    arc = row_chunk(block_rows)

    def sum_rows(i, carry):
        squares, largest = carry
        r = pl.ds(pl.multiple_of(i * arc, arc), arc)
        for c in range(a_width // a_chunk):
            cols = slice(c * a_chunk, (c + 1) * a_chunk)
            x = arep[0, r, cols].astype(jnp.float32)
            for k in range(1, n_out):
                x = x + arep[k, r, cols].astype(jnp.float32)
            asum[r, cols] = x
            squares = squares + x * x
            largest = jnp.maximum(largest, jnp.abs(x))
        return squares, largest

    zeros = jnp.zeros((arc, a_chunk), jnp.float32)
    a_sq, a_max = lax.fori_loop(0, block_rows // arc, sum_rows, (zeros, zeros))
    total = jnp.sum(e_sq) + jnp.sum(a_sq)
    part[0] = jnp.full(part.shape[1:], total, jnp.float32)

    sq_out = []
    for k in send_order(n_out):
        c = remote(part.at[0], part.at[k], p_send.at[k], p_recv.at[k], to_out(k))
        c.start()
        sq_out.append(c)
    largest = jnp.maximum(jnp.max(a_max), 1e-30)
    scale = jnp.full((1, 1), top, jnp.float32) / largest

    def code_rows(i, _):
        r = pl.ds(pl.multiple_of(i * arc, arc), arc)
        for c in range(a_width // a_chunk):
            cols = slice(c * a_chunk, (c + 1) * a_chunk)
            acode[r, cols] = encode(asum[r, cols] * scale).astype(jnp.bfloat16)
        return 0

    lax.fori_loop(0, block_rows // arc, code_rows, 0)
    own_rows = pltpu.make_async_copy(rows_at(acode, in_me, a_rows), agot.at[0], own_sem.at[2])
    own_rows.start()
    own_grad = pltpu.make_async_copy(rows_at(mine, in_me, rows), held.at[0], own_sem.at[3])
    own_grad.start()
    for c in sq_out:
        c.wait()
    total = jnp.sum(part[:n_out, 0:1, 0:1])
    acc[0, 0:4] = jnp.full((4, acc.shape[2]), total, jnp.float32)
    acc[0, 4:8] = jnp.full((4, acc.shape[2]), largest, jnp.float32)
    sq_in = []
    for k in order:
        c = remote(acc.at[0], acc.at[k], q_send.at[k], q_recv.at[k], to_in(k))
        c.start()
        sq_in.append(c)
    attn_fwd = {}
    for k in order:
        c = remote(
            rows_at(acode, partner_to(in_me, k, n_in), a_rows), agot.at[k],
            h_send.at[k], h_recv.at[k], to_in(k),
        )
        c.start()
        attn_fwd[k] = c
    for k in rest:
        send_fwd(k)
    for c in sq_in:
        c.wait()
    total = jnp.sum(acc[:n_in, 0:1, 0:1])
    clip = 1.0 / jnp.sqrt(jnp.full((1, 1), total, jnp.float32) / numel + 1e-06)

    own_rows.wait()
    for c in state:
        c.wait()
    arow = row_chunk(a_rows)

    def update(k, source, held, factor, load, refs, n_rows, n_cols, cc, rchunk):
        master, moment, second = refs

        def body(i, _):
            r = pl.ds(pl.multiple_of(i * rchunk, rchunk), rchunk)
            for c in range(n_cols // cc):
                cols = pl.ds(pl.multiple_of(source * n_cols + c * cc, 128), cc)
                here = slice(c * cc, (c + 1) * cc)
                g = load(held[k, r, here].astype(jnp.float32))
                a, b, d = adam_update(g, master[r, cols], moment[r, cols], second[r, cols], factor)
                master[r, cols] = a
                moment[r, cols] = b
                second[r, cols] = d
                held[k, r, here] = a.astype(jnp.bfloat16)
            return 0

        lax.fori_loop(0, n_rows // rchunk, body, 0)

    block_base = out_me * block_rows

    def attn_place(owner):
        return aw_o.at[pl.ds(pl.multiple_of(block_base + owner * a_rows, a_rows), a_rows)]

    attn_back = []
    attn_refs = (am_o, ao_o, as_o)
    for k in order + [0]:
        if k:
            attn_fwd[k].wait_recv()
        factor = clip * (acc[k, 4:5, 0:1] / top)
        update(
            k, partner_from(in_me, k, n_in), agot, factor, decode, attn_refs,
            a_rows, a_width, a_chunk, arow,
        )
    for k in order:
        where = (out_me, partner_from(in_me, k, n_in))
        c = remote(agot.at[k], attn_place(in_me), r_send.at[k], r_recv.at[k], where)
        c.start()
        attn_back.append(c)
    attn_own = pltpu.make_async_copy(agot.at[0], attn_place(in_me), own_sem.at[4])
    attn_own.start()

    erow = row_chunk(rows)
    e_refs = (em_o, eo_o, es_o)
    back = []
    gather = []
    for k in arrival:
        if k:
            fwd[k].wait_recv()
        else:
            own_grad.wait()
        update(
            k, partner_from(in_me, k, n_in), held, clip, lambda g: g, e_refs,
            rows, width, chunk, erow,
        )
        if k:
            where = (out_me, partner_from(in_me, k, n_in))
            c = remote(held.at[k], rows_at(ew_o, in_me, rows), s_send.at[k], s_recv.at[k], where)
            c.start()
            back.append(c)
        else:
            own_weight = pltpu.make_async_copy(held.at[0], rows_at(ew_o, in_me, rows), own_sem.at[5])
            own_weight.start()
    attn_own.wait()
    for c in attn_back:
        c.wait_recv()
    for k in send_order(n_out):
        mine_rows = rows_at(aw_o, out_me, block_rows)
        c = remote(mine_rows, mine_rows, t_send.at[k], t_recv.at[k], to_out(k))
        c.start()
        gather.append(c)

    for k in order:
        fwd[k].wait_send()
        attn_fwd[k].wait_send()
    for k in send_order(n_out):
        rep_copies[k].wait_send()
    for c in attn_back:
        c.wait_send()
    own_weight.wait()
    for c in gather:
        c.wait()
    for c in back:
        c.wait()


def put_kernel(*refs):
    count = (len(refs) - 1) // 2
    sem = refs[-1]
    copies = [
        pltpu.make_async_copy(refs[i], refs[count + i], sem.at[i]) for i in range(count)
    ]
    for c in copies:
        c.start()
    for c in copies:
        c.wait()


def local(n_out, n_in, eg, ag, em, eo, es, am, ao, as_):
    experts, e_rows, width = eg.shape
    eg = eg.reshape(experts * e_rows, width)
    ag = ag.reshape(ag.shape[1], ag.shape[2])
    numel = (em.shape[0] * em.shape[1] + am.shape[0] * am.shape[1]) * n_out * n_in
    rows = em.shape[0]
    a_rows = am.shape[0]
    a_width = ag.shape[1]
    block_rows = ag.shape[0] // n_out
    f32, bf16 = jnp.float32, jnp.bfloat16
    shapes = [(em.shape, f32)] * 3 + [(am.shape, f32)] * 3 + [(eg.shape, bf16), (ag.shape, bf16)]
    any_spec = pl.BlockSpec(memory_space=pl.ANY)
    vmem_spec = pl.BlockSpec(memory_space=pltpu.VMEM)
    dma = pltpu.SemaphoreType.DMA
    out = pl.pallas_call(
        functools.partial(step_kernel, n_out, n_in, float(numel)),
        out_shape=[pltpu.VMEM(s, d) for s, d in shapes],
        in_specs=[pl.BlockSpec(memory_space=pltpu.HBM)] * 8,
        out_specs=[vmem_spec] * 8,
        scratch_shapes=[
            pltpu.VMEM(eg.shape, bf16),
            pltpu.VMEM((n_in, rows, width), bf16),
            pltpu.VMEM((n_out, block_rows, a_width), bf16),
            pltpu.VMEM((block_rows, a_width), f32),
            pltpu.VMEM((block_rows, a_width), bf16),
            pltpu.VMEM((n_in, a_rows, a_width), bf16),
            pltpu.VMEM((n_out, 8, 128), f32),
            pltpu.VMEM((n_in, 8, 128), f32),
            dma((6,)), dma((6,)),
            dma((n_in,)), dma((n_in,)),
            dma((n_out,)), dma((n_out,)),
            dma((n_in,)), dma((n_in,)),
            dma((n_out,)), dma((n_out,)),
            dma((n_in,)), dma((n_in,)),
            dma((n_in,)), dma((n_in,)),
            dma((n_in,)), dma((n_in,)),
            dma((n_out,)), dma((n_out,)),
        ],
        compiler_params=pltpu.CompilerParams(
            collective_id=0, has_side_effects=True, vmem_limit_bytes=26 * 1024 * 1024
        ),
    )(eg, ag, em, eo, es, am, ao, as_)
    out = pl.pallas_call(
        put_kernel,
        out_shape=[jax.ShapeDtypeStruct(x.shape, x.dtype) for x in out],
        in_specs=[vmem_spec] * 8,
        out_specs=[any_spec] * 8,
        scratch_shapes=[dma((8,))],
        compiler_params=pltpu.CompilerParams(vmem_limit_bytes=1024 * 1024),
    )(*out)
    return (*out[:6], out[6].reshape(experts, e_rows, width), out[7])


def solution(mesh):
    grouped = P(("gx", "gy"), None)
    in_specs = (P("gx", None, "gy"), P("gx", None, "gy")) + (grouped,) * 6
    out_specs = (grouped,) * 6 + (P("gx", None, "gy"), P(None, "gy"))
    step = functools.partial(local, mesh.shape["gx"], mesh.shape["gy"])
    return jax.shard_map(step, mesh=mesh, in_specs=in_specs, out_specs=out_specs, check_vma=False)
```

```python
import functools
import math

import jax
import jax.numpy as jnp
from jax import lax
from jax.experimental import pallas as pl
from jax.experimental.pallas import tpu as pltpu
from jax.sharding import PartitionSpec as P

MESH = pl.DeviceIdType.MESH

beta_one = 0.9
beta_two = 0.95
learn_rate = 0.01
weight_decay = 0.1
adam_eps = 1e-08
bias_one = 1.0 - 0.9**20
bias_two = 1.0 - 0.95**20


def adam_update(gradient, master, moment, second, clip_factor):
    scaled = clip_factor * gradient
    moment_new = beta_one * moment + (1.0 - beta_one) * scaled
    second_new = beta_two * second + (1.0 - beta_two) * scaled * scaled
    update = moment_new / bias_one / (jnp.sqrt(second_new / bias_two) + adam_eps)
    master_new = master - learn_rate * (update + weight_decay * master)
    return (master_new, moment_new, second_new)


def partner_to(me, k, n):
    if n & (n - 1):
        return lax.rem(me + k, n)
    out, bit = me, 1
    while bit < n:
        if k & bit:
            out = out + bit * (1 - 2 * lax.rem(me // bit, 2))
        bit *= 2
    return out


def partner_from(me, k, n):
    if n & (n - 1):
        return lax.rem(me + n - k, n)
    return partner_to(me, k, n)


def send_order(n):
    return list(range(n - 1, 0, -1))


def col_chunk(width):
    return 256 if width % 256 == 0 else 128


def row_chunk(rows):
    return math.gcd(rows, 16)


def partner_of(me, k, n):
    return (me + k) % n if n & (n - 1) else me ^ k


def far_blocks(n):
    return [n - 2]


def kept_rows(rows):
    return max(rows * 6 // 8 // 16 * 16, 16) if rows > 16 else rows // 2


top = 2.0**15.5
floor = 2.0**-15.5


def encode(x):
    square = x * x
    fourth = square * square
    eighth = jnp.where(jnp.abs(x) < floor, 0.0, fourth * fourth)
    return jnp.where(x < 0.0, -eighth, eighth)


def decode(y):
    root = jnp.sqrt(jnp.sqrt(jnp.sqrt(jnp.abs(y))))
    return jnp.where(y < 0.0, -root, root)


def step_kernel(
    n_out, n_in, numel,
    eg, ag, em, eo, es, am, ao, as_,
    em_o, eo_o, es_o, am_o, ao_o, as_o, ew_o, aw_o, left,
    mine, held, arep, asum, acode, agot, part, acc,
    own_sem, state_sem, f_send, f_recv, g_send, g_recv, h_send, h_recv,
    p_send, p_recv, q_send, q_recv, r_send, r_recv, s_send, s_recv, t_send, t_recv,
):
    out_me = lax.axis_index("gx")
    in_me = lax.axis_index("gy")
    rows, width = held.shape[1], held.shape[2]
    block_rows, a_width = arep.shape[1], arep.shape[2]
    a_rows = agot.shape[1]

    def to_in(k):
        return (out_me, partner_to(in_me, k, n_in))

    def to_out(k):
        return (partner_to(out_me, k, n_out), in_me)

    def remote(src, dst, send, recv, where):
        return pltpu.make_async_remote_copy(
            src_ref=src, dst_ref=dst, send_sem=send, recv_sem=recv,
            device_id=where, device_id_type=MESH,
        )

    def rows_at(ref, index, count):
        return ref.at[pl.ds(pl.multiple_of(index * count, count), count)]

    barrier = pltpu.get_barrier_semaphore()
    for k in range(1, n_in):
        pl.semaphore_signal(barrier, inc=1, device_id=to_in(k), device_id_type=MESH)
    for k in range(1, n_out):
        pl.semaphore_signal(barrier, inc=1, device_id=to_out(k), device_id_type=MESH)

    load_grad = pltpu.make_async_copy(eg, mine, own_sem.at[0])
    load_grad.start()
    load_rep = pltpu.make_async_copy(rows_at(ag, out_me, block_rows), arep.at[0], own_sem.at[1])
    load_rep.start()
    pl.semaphore_wait(barrier, n_in - 1 + n_out - 1)

    rep_copies = {}
    for k in send_order(n_out):
        c = remote(
            rows_at(ag, partner_to(out_me, k, n_out), block_rows), arep.at[k],
            g_send.at[k], g_recv.at[k], to_out(k),
        )
        c.start()
        rep_copies[k] = c
    order = send_order(n_in)
    far, near = order[: n_in // 2], order[n_in // 2 :]
    first = far[: n_in // 4] + near[:1]
    rest = near[1:] + far[n_in // 4 :]
    arrival = first + near[1:] + [0] + far[n_in // 4 :]
    fwd = {}

    def send_fwd(k):
        c = remote(
            rows_at(eg, partner_to(in_me, k, n_in), rows), held.at[k],
            f_send.at[k], f_recv.at[k], to_in(k),
        )
        c.start()
        fwd[k] = c

    for k in first:
        send_fwd(k)

    state = []
    for i, (src, dst) in enumerate(
        ((em, em_o), (eo, eo_o), (es, es_o), (am, am_o), (ao, ao_o), (as_, as_o))
    ):
        c = pltpu.make_async_copy(src, dst, state_sem.at[i])
        c.start()
        state.append(c)

    load_grad.wait()
    chunk = col_chunk(width)
    rc = row_chunk(mine.shape[0])

    def square_rows(i, carry):
        r = pl.ds(pl.multiple_of(i * rc, rc), rc)
        for c in range(width // chunk):
            x = mine[r, c * chunk : (c + 1) * chunk].astype(jnp.float32)
            carry = carry + x * x
        return carry

    e_sq = lax.fori_loop(0, mine.shape[0] // rc, square_rows, jnp.zeros((rc, chunk), jnp.float32))

    load_rep.wait()
    for k in send_order(n_out):
        rep_copies[k].wait_recv()
    a_chunk = col_chunk(a_width)
    arc = row_chunk(block_rows)

    def sum_rows(i, carry):
        squares, largest = carry
        r = pl.ds(pl.multiple_of(i * arc, arc), arc)
        for c in range(a_width // a_chunk):
            cols = slice(c * a_chunk, (c + 1) * a_chunk)
            x = arep[0, r, cols].astype(jnp.float32)
            for k in range(1, n_out):
                x = x + arep[k, r, cols].astype(jnp.float32)
            asum[r, cols] = x
            squares = squares + x * x
            largest = jnp.maximum(largest, jnp.abs(x))
        return squares, largest

    zeros = jnp.zeros((arc, a_chunk), jnp.float32)
    a_sq, a_max = lax.fori_loop(0, block_rows // arc, sum_rows, (zeros, zeros))
    total = jnp.sum(e_sq) + jnp.sum(a_sq)
    part[0] = jnp.full(part.shape[1:], total, jnp.float32)

    sq_out = []
    for k in send_order(n_out):
        c = remote(part.at[0], part.at[k], p_send.at[k], p_recv.at[k], to_out(k))
        c.start()
        sq_out.append(c)
    largest = jnp.maximum(jnp.max(a_max), 1e-30)
    scale = jnp.full((1, 1), top, jnp.float32) / largest

    def code_rows(i, _):
        r = pl.ds(pl.multiple_of(i * arc, arc), arc)
        for c in range(a_width // a_chunk):
            cols = slice(c * a_chunk, (c + 1) * a_chunk)
            acode[r, cols] = encode(asum[r, cols] * scale).astype(jnp.bfloat16)
        return 0

    lax.fori_loop(0, block_rows // arc, code_rows, 0)
    own_rows = pltpu.make_async_copy(rows_at(acode, in_me, a_rows), agot.at[0], own_sem.at[2])
    own_rows.start()
    own_grad = pltpu.make_async_copy(rows_at(mine, in_me, rows), held.at[0], own_sem.at[3])
    own_grad.start()
    for c in sq_out:
        c.wait()
    total = jnp.sum(part[:n_out, 0:1, 0:1])
    acc[0, 0:4] = jnp.full((4, acc.shape[2]), total, jnp.float32)
    acc[0, 4:8] = jnp.full((4, acc.shape[2]), largest, jnp.float32)
    sq_in = []
    for k in order:
        c = remote(acc.at[0], acc.at[k], q_send.at[k], q_recv.at[k], to_in(k))
        c.start()
        sq_in.append(c)
    attn_fwd = {}
    for k in order:
        c = remote(
            rows_at(acode, partner_to(in_me, k, n_in), a_rows), agot.at[k],
            h_send.at[k], h_recv.at[k], to_in(k),
        )
        c.start()
        attn_fwd[k] = c
    for k in rest:
        send_fwd(k)
    for c in sq_in:
        c.wait()
    total = jnp.sum(acc[:n_in, 0:1, 0:1])
    clip = 1.0 / jnp.sqrt(jnp.full((1, 1), total, jnp.float32) / numel + 1e-06)

    own_rows.wait()
    for c in state:
        c.wait()
    arow = row_chunk(a_rows)

    def update(k, source, held, factor, load, refs, n_rows, n_cols, cc, rchunk):
        master, moment, second = refs

        def body(i, _):
            r = pl.ds(pl.multiple_of(i * rchunk, rchunk), rchunk)
            for c in range(n_cols // cc):
                cols = pl.ds(pl.multiple_of(source * n_cols + c * cc, 128), cc)
                here = slice(c * cc, (c + 1) * cc)
                g = load(held[k, r, here].astype(jnp.float32))
                a, b, d = adam_update(g, master[r, cols], moment[r, cols], second[r, cols], factor)
                master[r, cols] = a
                moment[r, cols] = b
                second[r, cols] = d
                held[k, r, here] = a.astype(jnp.bfloat16)
            return 0

        lax.fori_loop(0, n_rows // rchunk, body, 0)

    block_base = out_me * block_rows

    def attn_place(owner):
        return aw_o.at[pl.ds(pl.multiple_of(block_base + owner * a_rows, a_rows), a_rows)]

    attn_back = []
    attn_refs = (am_o, ao_o, as_o)
    for k in order + [0]:
        if k:
            attn_fwd[k].wait_recv()
        factor = clip * (acc[k, 4:5, 0:1] / top)
        update(
            k, partner_from(in_me, k, n_in), agot, factor, decode, attn_refs,
            a_rows, a_width, a_chunk, arow,
        )
    for k in order:
        where = (out_me, partner_from(in_me, k, n_in))
        c = remote(agot.at[k], attn_place(in_me), r_send.at[k], r_recv.at[k], where)
        c.start()
        attn_back.append(c)
    attn_own = pltpu.make_async_copy(agot.at[0], attn_place(in_me), own_sem.at[4])
    attn_own.start()

    erow = row_chunk(rows)
    e_refs = (em_o, eo_o, es_o)
    back = []
    gather = []
    for k in arrival:
        if k:
            fwd[k].wait_recv()
        else:
            own_grad.wait()
        update(
            k, partner_from(in_me, k, n_in), held, clip, lambda g: g, e_refs,
            rows, width, chunk, erow,
        )
        if k:
            where = (out_me, partner_from(in_me, k, n_in))
            sent = rows
            if k in far_blocks(n_in):
                keep = kept_rows(rows)
                sent = rows - keep
                left[far_blocks(n_in).index(k)] = held[k, sent:rows]
            place = pl.ds(pl.multiple_of(in_me * rows, rows), sent)
            c = remote(held.at[k, 0:sent], ew_o.at[place], s_send.at[k], s_recv.at[k], where)
            c.start()
            back.append(c)
        else:
            own_weight = pltpu.make_async_copy(held.at[0], rows_at(ew_o, in_me, rows), own_sem.at[5])
            own_weight.start()
    attn_own.wait()
    for c in attn_back:
        c.wait_recv()
    for k in send_order(n_out):
        mine_rows = rows_at(aw_o, out_me, block_rows)
        c = remote(mine_rows, mine_rows, t_send.at[k], t_recv.at[k], to_out(k))
        c.start()
        gather.append(c)

    for k in order:
        fwd[k].wait_send()
        attn_fwd[k].wait_send()
    for k in send_order(n_out):
        rep_copies[k].wait_send()
    for c in attn_back:
        c.wait_send()
    own_weight.wait()
    for c in gather:
        c.wait()
    for c in back:
        c.wait()


def put_kernel(*refs):
    count = (len(refs) - 1) // 2
    sem = refs[-1]
    copies = [
        pltpu.make_async_copy(refs[i], refs[count + i], sem.at[i]) for i in range(count)
    ]
    for c in copies:
        c.start()
    for c in copies:
        c.wait()


def last_kernel(n_in, rows, *refs):
    count = len(refs) - 3
    out, sem = refs[-2:]
    in_me = lax.axis_index("gy")
    copies = []
    for i, k in enumerate(far_blocks(n_in)):
        keep = refs[1 + i].shape[0]
        start = partner_to(in_me, k, n_in) * rows + (rows - keep)
        place = pl.ds(pl.multiple_of(start, math.gcd(rows, keep)), keep)
        copies.append(pltpu.make_async_copy(refs[1 + i], out.at[place], sem.at[i]))
    for c in copies:
        c.start()
    for c in copies:
        c.wait()


def local(n_out, n_in, eg, ag, em, eo, es, am, ao, as_):
    experts, e_rows, width = eg.shape
    eg = eg.reshape(experts * e_rows, width)
    ag = ag.reshape(ag.shape[1], ag.shape[2])
    numel = (em.shape[0] * em.shape[1] + am.shape[0] * am.shape[1]) * n_out * n_in
    rows = em.shape[0]
    a_rows = am.shape[0]
    a_width = ag.shape[1]
    block_rows = ag.shape[0] // n_out
    f32, bf16 = jnp.float32, jnp.bfloat16
    shapes = [(em.shape, f32)] * 3 + [(am.shape, f32)] * 3 + [(eg.shape, bf16), (ag.shape, bf16)]
    far = far_blocks(n_in)
    shapes += [((len(far), kept_rows(rows), width), bf16)]
    any_spec = pl.BlockSpec(memory_space=pl.ANY)
    vmem_spec = pl.BlockSpec(memory_space=pltpu.VMEM)
    dma = pltpu.SemaphoreType.DMA
    out = pl.pallas_call(
        functools.partial(step_kernel, n_out, n_in, float(numel)),
        out_shape=[pltpu.VMEM(s, d) for s, d in shapes],
        in_specs=[pl.BlockSpec(memory_space=pltpu.HBM)] * 8,
        out_specs=[vmem_spec] * 9,
        scratch_shapes=[
            pltpu.VMEM(eg.shape, bf16),
            pltpu.VMEM((n_in, rows, width), bf16),
            pltpu.VMEM((n_out, block_rows, a_width), bf16),
            pltpu.VMEM((block_rows, a_width), f32),
            pltpu.VMEM((block_rows, a_width), bf16),
            pltpu.VMEM((n_in, a_rows, a_width), bf16),
            pltpu.VMEM((n_out, 8, 128), f32),
            pltpu.VMEM((n_in, 8, 128), f32),
            dma((6,)), dma((6,)),
            dma((n_in,)), dma((n_in,)),
            dma((n_out,)), dma((n_out,)),
            dma((n_in,)), dma((n_in,)),
            dma((n_out,)), dma((n_out,)),
            dma((n_in,)), dma((n_in,)),
            dma((n_in,)), dma((n_in,)),
            dma((n_in,)), dma((n_in,)),
            dma((n_out,)), dma((n_out,)),
        ],
        compiler_params=pltpu.CompilerParams(
            collective_id=0, has_side_effects=True, vmem_limit_bytes=26 * 1024 * 1024
        ),
    )(eg, ag, em, eo, es, am, ao, as_)
    *out, left = out
    came = [
        lax.ppermute(left[i], "gy", [(j, partner_of(j, k, n_in)) for j in range(n_in)])
        for i, k in enumerate(far)
    ]
    moved = sum(x.size * x.dtype.itemsize for x in out)
    out = pl.pallas_call(
        put_kernel,
        out_shape=[jax.ShapeDtypeStruct(x.shape, x.dtype) for x in out],
        in_specs=[vmem_spec] * 8,
        out_specs=[any_spec] * 8,
        scratch_shapes=[dma((8,))],
        compiler_params=pltpu.CompilerParams(vmem_limit_bytes=1024 * 1024),
        cost_estimate=pl.CostEstimate(flops=0, bytes_accessed=2 * moved, transcendentals=0),
    )(*out)
    out = list(out)
    out[6] = pl.pallas_call(
        functools.partial(last_kernel, n_in, rows),
        out_shape=jax.ShapeDtypeStruct(out[6].shape, bf16),
        in_specs=[any_spec] + [vmem_spec] * len(far),
        out_specs=any_spec,
        scratch_shapes=[dma((len(far),))],
        input_output_aliases={0: 0},
        compiler_params=pltpu.CompilerParams(vmem_limit_bytes=1024 * 1024),
    )(out[6], *came)
    return (*out[:6], out[6].reshape(experts, e_rows, width), out[7])


def solution(mesh):
    grouped = P(("gx", "gy"), None)
    in_specs = (P("gx", None, "gy"), P("gx", None, "gy")) + (grouped,) * 6
    out_specs = (grouped,) * 6 + (P("gx", None, "gy"), P(None, "gy"))
    step = functools.partial(local, mesh.shape["gx"], mesh.shape["gy"])
    return jax.shard_map(step, mesh=mesh, in_specs=in_specs, out_specs=out_specs, check_vma=False)
```

```python
import functools
import math

import jax
import jax.numpy as jnp
from jax import lax
from jax.experimental import pallas as pl
from jax.experimental.pallas import tpu as pltpu
from jax.sharding import PartitionSpec as P

MESH = pl.DeviceIdType.MESH

beta_one = 0.9
beta_two = 0.95
learn_rate = 0.01
weight_decay = 0.1
adam_eps = 1e-08
bias_one = 1.0 - 0.9**20
bias_two = 1.0 - 0.95**20


def adam_update(gradient, master, moment, second, clip_factor):
    scaled = clip_factor * gradient
    moment_new = beta_one * moment + (1.0 - beta_one) * scaled
    second_new = beta_two * second + (1.0 - beta_two) * scaled * scaled
    update = moment_new / bias_one / (jnp.sqrt(second_new / bias_two) + adam_eps)
    master_new = master - learn_rate * (update + weight_decay * master)
    return (master_new, moment_new, second_new)


def partner_to(me, k, n):
    if n & (n - 1):
        return lax.rem(me + k, n)
    out, bit = me, 1
    while bit < n:
        if k & bit:
            out = out + bit * (1 - 2 * lax.rem(me // bit, 2))
        bit *= 2
    return out


def partner_from(me, k, n):
    if n & (n - 1):
        return lax.rem(me + n - k, n)
    return partner_to(me, k, n)


def send_order(n):
    return list(range(n - 1, 0, -1))


def col_chunk(width):
    return 256 if width % 256 == 0 else 128


def row_chunk(rows):
    return math.gcd(rows, 16)


def partner_of(me, k, n):
    return (me + k) % n if n & (n - 1) else me ^ k


def far_blocks(n):
    return [n - 2]


def kept_rows(rows):
    return max(rows * 5 // 8 // 16 * 16, 16) if rows > 16 else rows // 2


top = 2.0**15.5
floor = 2.0**-15.5


def encode(x):
    square = x * x
    fourth = square * square
    eighth = jnp.where(jnp.abs(x) < floor, 0.0, fourth * fourth)
    return jnp.where(x < 0.0, -eighth, eighth)


def decode(y):
    root = jnp.sqrt(jnp.sqrt(jnp.sqrt(jnp.abs(y))))
    return jnp.where(y < 0.0, -root, root)


def step_kernel(
    n_out, n_in, numel,
    eg, ag, em, eo, es, am, ao, as_,
    em_o, eo_o, es_o, am_o, ao_o, as_o, ew_o, aw_o, left,
    mine, held, arep, asum, acode, agot, part, acc,
    ready, own_sem, load_sem, state_sem, f_send, f_recv, g_send, g_recv, h_send, h_recv,
    p_send, p_recv, q_send, q_recv, r_send, r_recv, s_send, s_recv, t_send, t_recv,
):
    out_me = lax.axis_index("gx")
    in_me = lax.axis_index("gy")
    rows, width = held.shape[1], held.shape[2]
    block_rows, a_width = arep.shape[1], arep.shape[2]
    a_rows = agot.shape[1]

    def to_in(k):
        return (out_me, partner_to(in_me, k, n_in))

    def to_out(k):
        return (partner_to(out_me, k, n_out), in_me)

    def remote(src, dst, send, recv, where):
        return pltpu.make_async_remote_copy(
            src_ref=src, dst_ref=dst, send_sem=send, recv_sem=recv,
            device_id=where, device_id_type=MESH,
        )

    def rows_at(ref, index, count):
        return ref.at[pl.ds(pl.multiple_of(index * count, count), count)]

    barrier = pltpu.get_barrier_semaphore()

    def signal(sem, where):
        pl.semaphore_signal(sem, inc=1, device_id=where, device_id_type=MESH)

    quarter = n_in // 4
    staged = quarter > 0 and not n_in & (n_in - 1)
    middle = outer = None
    if staged:
        middle = lax.rem(in_me // quarter, 2) != in_me // (2 * quarter)
        outer = jnp.logical_not(middle)
        for k in range(3 * quarter, n_in):
            signal(barrier, to_in(k))

        @pl.when(middle)
        def _():
            for k in range(quarter, 3 * quarter):
                signal(barrier, to_in(k))

        @pl.when(outer)
        def _():
            for k in range(1, quarter):
                signal(barrier, to_in(k))
            for k in range(1, n_out):
                signal(barrier, to_out(k))
    else:
        for k in range(1, n_in):
            signal(barrier, to_in(k))
        for k in range(1, n_out):
            signal(barrier, to_out(k))

    order = send_order(n_in)
    far, near = order[: n_in // 2], order[n_in // 2 :]
    first = far[: n_in // 4] + near[:1]
    rest = near[1:] + far[n_in // 4 :]
    arrival = first + near[1:] + [0] + far[n_in // 4 :]

    def block_of(ref, k):
        return rows_at(ref, partner_to(in_me, k, n_in), rows)

    load = {}
    for k in first + rest + [0]:
        load[k] = pltpu.make_async_copy(block_of(eg, k), block_of(mine, k), load_sem.at[k])
        load[k].start()
    load_rep = pltpu.make_async_copy(rows_at(ag, out_me, block_rows), arep.at[0], own_sem.at[1])
    load_rep.start()
    everyone = n_in - 1 + n_out - 1
    if staged:
        @pl.when(middle)
        def _():
            pl.semaphore_wait(barrier, quarter)

        @pl.when(outer)
        def _():
            pl.semaphore_wait(barrier, everyone)
    else:
        pl.semaphore_wait(barrier, everyone)

    fwd = {}

    def send_fwd(k):
        c = remote(block_of(mine, k), held.at[k], f_send.at[k], f_recv.at[k], to_in(k))
        c.start()
        fwd[k] = c

    for k in far[:quarter]:
        load[k].wait()
        send_fwd(k)
    if staged:
        @pl.when(outer)
        def _():
            for k in range(1, n_out):
                signal(ready, to_out(k))
            if n_out > 1:
                pl.semaphore_wait(ready, n_out - 1)
            signal(ready, to_in(quarter))

        @pl.when(middle)
        def _():
            pl.semaphore_wait(ready, 1)

    rep_copies = {}
    for k in send_order(n_out):
        c = remote(
            rows_at(ag, partner_to(out_me, k, n_out), block_rows), arep.at[k],
            g_send.at[k], g_recv.at[k], to_out(k),
        )
        c.start()
        rep_copies[k] = c
    for k in near[:1]:
        load[k].wait()
        send_fwd(k)

    state = []
    for i, (src, dst) in enumerate(
        ((em, em_o), (eo, eo_o), (es, es_o), (am, am_o), (ao, ao_o), (as_, as_o))
    ):
        c = pltpu.make_async_copy(src, dst, state_sem.at[i])
        c.start()
        state.append(c)

    for k in rest + [0]:
        load[k].wait()
    chunk = col_chunk(width)
    rc = row_chunk(mine.shape[0])

    def square_rows(i, carry):
        r = pl.ds(pl.multiple_of(i * rc, rc), rc)
        for c in range(width // chunk):
            x = mine[r, c * chunk : (c + 1) * chunk].astype(jnp.float32)
            carry = carry + x * x
        return carry

    e_sq = lax.fori_loop(0, mine.shape[0] // rc, square_rows, jnp.zeros((rc, chunk), jnp.float32))

    load_rep.wait()
    for k in send_order(n_out):
        rep_copies[k].wait_recv()
    a_chunk = col_chunk(a_width)
    arc = row_chunk(block_rows)

    def sum_rows(i, carry):
        squares, largest = carry
        r = pl.ds(pl.multiple_of(i * arc, arc), arc)
        for c in range(a_width // a_chunk):
            cols = slice(c * a_chunk, (c + 1) * a_chunk)
            x = arep[0, r, cols].astype(jnp.float32)
            for k in range(1, n_out):
                x = x + arep[k, r, cols].astype(jnp.float32)
            asum[r, cols] = x
            squares = squares + x * x
            largest = jnp.maximum(largest, jnp.abs(x))
        return squares, largest

    zeros = jnp.zeros((arc, a_chunk), jnp.float32)
    a_sq, a_max = lax.fori_loop(0, block_rows // arc, sum_rows, (zeros, zeros))
    total = jnp.sum(e_sq) + jnp.sum(a_sq)
    part[0] = jnp.full(part.shape[1:], total, jnp.float32)

    sq_out = []
    for k in send_order(n_out):
        c = remote(part.at[0], part.at[k], p_send.at[k], p_recv.at[k], to_out(k))
        c.start()
        sq_out.append(c)
    largest = jnp.maximum(jnp.max(a_max), 1e-30)
    scale = jnp.full((1, 1), top, jnp.float32) / largest

    def code_rows(i, _):
        r = pl.ds(pl.multiple_of(i * arc, arc), arc)
        for c in range(a_width // a_chunk):
            cols = slice(c * a_chunk, (c + 1) * a_chunk)
            acode[r, cols] = encode(asum[r, cols] * scale).astype(jnp.bfloat16)
        return 0

    lax.fori_loop(0, block_rows // arc, code_rows, 0)
    own_rows = pltpu.make_async_copy(rows_at(acode, in_me, a_rows), agot.at[0], own_sem.at[2])
    own_rows.start()
    own_grad = pltpu.make_async_copy(rows_at(mine, in_me, rows), held.at[0], own_sem.at[3])
    own_grad.start()
    for c in sq_out:
        c.wait()
    total = jnp.sum(part[:n_out, 0:1, 0:1])
    acc[0, 0:4] = jnp.full((4, acc.shape[2]), total, jnp.float32)
    acc[0, 4:8] = jnp.full((4, acc.shape[2]), largest, jnp.float32)
    sq_in = []
    for k in order:
        c = remote(acc.at[0], acc.at[k], q_send.at[k], q_recv.at[k], to_in(k))
        c.start()
        sq_in.append(c)
    attn_fwd = {}
    for k in order:
        c = remote(
            rows_at(acode, partner_to(in_me, k, n_in), a_rows), agot.at[k],
            h_send.at[k], h_recv.at[k], to_in(k),
        )
        c.start()
        attn_fwd[k] = c
    for k in rest:
        send_fwd(k)
    for c in sq_in:
        c.wait()
    total = jnp.sum(acc[:n_in, 0:1, 0:1])
    clip = 1.0 / jnp.sqrt(jnp.full((1, 1), total, jnp.float32) / numel + 1e-06)

    own_rows.wait()
    for c in state:
        c.wait()
    arow = row_chunk(a_rows)

    def update(k, source, held, factor, load, refs, n_rows, n_cols, cc, rchunk):
        master, moment, second = refs

        def body(i, _):
            r = pl.ds(pl.multiple_of(i * rchunk, rchunk), rchunk)
            for c in range(n_cols // cc):
                cols = pl.ds(pl.multiple_of(source * n_cols + c * cc, 128), cc)
                here = slice(c * cc, (c + 1) * cc)
                g = load(held[k, r, here].astype(jnp.float32))
                a, b, d = adam_update(g, master[r, cols], moment[r, cols], second[r, cols], factor)
                master[r, cols] = a
                moment[r, cols] = b
                second[r, cols] = d
                held[k, r, here] = a.astype(jnp.bfloat16)
            return 0

        lax.fori_loop(0, n_rows // rchunk, body, 0)

    block_base = out_me * block_rows

    def attn_place(owner):
        return aw_o.at[pl.ds(pl.multiple_of(block_base + owner * a_rows, a_rows), a_rows)]

    attn_back = []
    attn_refs = (am_o, ao_o, as_o)
    for k in order + [0]:
        if k:
            attn_fwd[k].wait_recv()
        factor = clip * (acc[k, 4:5, 0:1] / top)
        update(
            k, partner_from(in_me, k, n_in), agot, factor, decode, attn_refs,
            a_rows, a_width, a_chunk, arow,
        )
    for k in order:
        where = (out_me, partner_from(in_me, k, n_in))
        c = remote(agot.at[k], attn_place(in_me), r_send.at[k], r_recv.at[k], where)
        c.start()
        attn_back.append(c)
    attn_own = pltpu.make_async_copy(agot.at[0], attn_place(in_me), own_sem.at[4])
    attn_own.start()

    erow = row_chunk(rows)
    e_refs = (em_o, eo_o, es_o)
    back = []
    gather = []
    for k in arrival:
        if k:
            fwd[k].wait_recv()
        else:
            own_grad.wait()
        update(
            k, partner_from(in_me, k, n_in), held, clip, lambda g: g, e_refs,
            rows, width, chunk, erow,
        )
        if k:
            where = (out_me, partner_from(in_me, k, n_in))
            sent = rows
            if k in far_blocks(n_in):
                sent = rows - kept_rows(rows)
                left[far_blocks(n_in).index(k)] = held[k, sent:rows]
            place = pl.ds(pl.multiple_of(in_me * rows, rows), sent)
            c = remote(held.at[k, 0:sent], ew_o.at[place], s_send.at[k], s_recv.at[k], where)
            if sent == rows:
                c.start()
            back.append(c)
        else:
            own_weight = pltpu.make_async_copy(held.at[0], rows_at(ew_o, in_me, rows), own_sem.at[5])
            own_weight.start()
    for k, c in zip([k for k in arrival if k], back):
        if k in far_blocks(n_in):
            c.start()
    attn_own.wait()
    for c in attn_back:
        c.wait_recv()
    for k in send_order(n_out):
        mine_rows = rows_at(aw_o, out_me, block_rows)
        c = remote(mine_rows, mine_rows, t_send.at[k], t_recv.at[k], to_out(k))
        c.start()
        gather.append(c)

    for k in order:
        fwd[k].wait_send()
        attn_fwd[k].wait_send()
    for k in send_order(n_out):
        rep_copies[k].wait_send()
    for c in attn_back:
        c.wait_send()
    own_weight.wait()
    for c in gather:
        c.wait()
    for c in back:
        c.wait()


def put_kernel(*refs):
    count = (len(refs) - 1) // 2
    sem = refs[-1]
    copies = [
        pltpu.make_async_copy(refs[i], refs[count + i], sem.at[i]) for i in range(count)
    ]
    for c in copies:
        c.start()
    for c in copies:
        c.wait()


def last_kernel(n_in, rows, *refs):
    count = len(refs) - 3
    out, sem = refs[-2:]
    in_me = lax.axis_index("gy")
    copies = []
    for i, k in enumerate(far_blocks(n_in)):
        keep = refs[1 + i].shape[0]
        start = partner_to(in_me, k, n_in) * rows + (rows - keep)
        place = pl.ds(pl.multiple_of(start, math.gcd(rows, keep)), keep)
        copies.append(pltpu.make_async_copy(refs[1 + i], out.at[place], sem.at[i]))
    for c in copies:
        c.start()
    for c in copies:
        c.wait()


def local(n_out, n_in, eg, ag, em, eo, es, am, ao, as_):
    experts, e_rows, width = eg.shape
    eg = eg.reshape(experts * e_rows, width)
    ag = ag.reshape(ag.shape[1], ag.shape[2])
    numel = (em.shape[0] * em.shape[1] + am.shape[0] * am.shape[1]) * n_out * n_in
    rows = em.shape[0]
    a_rows = am.shape[0]
    a_width = ag.shape[1]
    block_rows = ag.shape[0] // n_out
    f32, bf16 = jnp.float32, jnp.bfloat16
    shapes = [(em.shape, f32)] * 3 + [(am.shape, f32)] * 3 + [(eg.shape, bf16), (ag.shape, bf16)]
    far = far_blocks(n_in)
    shapes += [((len(far), kept_rows(rows), width), bf16)]
    any_spec = pl.BlockSpec(memory_space=pl.ANY)
    vmem_spec = pl.BlockSpec(memory_space=pltpu.VMEM)
    dma = pltpu.SemaphoreType.DMA
    out = pl.pallas_call(
        functools.partial(step_kernel, n_out, n_in, float(numel)),
        out_shape=[pltpu.VMEM(s, d) for s, d in shapes],
        in_specs=[pl.BlockSpec(memory_space=pltpu.HBM)] * 8,
        out_specs=[vmem_spec] * 9,
        scratch_shapes=[
            pltpu.VMEM(eg.shape, bf16),
            pltpu.VMEM((n_in, rows, width), bf16),
            pltpu.VMEM((n_out, block_rows, a_width), bf16),
            pltpu.VMEM((block_rows, a_width), f32),
            pltpu.VMEM((block_rows, a_width), bf16),
            pltpu.VMEM((n_in, a_rows, a_width), bf16),
            pltpu.VMEM((n_out, 8, 128), f32),
            pltpu.VMEM((n_in, 8, 128), f32),
            pltpu.SemaphoreType.REGULAR,
            dma((6,)), dma((n_in,)), dma((6,)),
            dma((n_in,)), dma((n_in,)),
            dma((n_out,)), dma((n_out,)),
            dma((n_in,)), dma((n_in,)),
            dma((n_out,)), dma((n_out,)),
            dma((n_in,)), dma((n_in,)),
            dma((n_in,)), dma((n_in,)),
            dma((n_in,)), dma((n_in,)),
            dma((n_out,)), dma((n_out,)),
        ],
        compiler_params=pltpu.CompilerParams(
            collective_id=0, has_side_effects=True, vmem_limit_bytes=26 * 1024 * 1024
        ),
    )(eg, ag, em, eo, es, am, ao, as_)
    *out, left = out
    came = [
        lax.ppermute(left[i], "gy", [(j, partner_of(j, k, n_in)) for j in range(n_in)])
        for i, k in enumerate(far)
    ]
    moved = sum(x.size * x.dtype.itemsize for x in out)
    out = pl.pallas_call(
        put_kernel,
        out_shape=[jax.ShapeDtypeStruct(x.shape, x.dtype) for x in out],
        in_specs=[vmem_spec] * 8,
        out_specs=[any_spec] * 8,
        scratch_shapes=[dma((8,))],
        compiler_params=pltpu.CompilerParams(vmem_limit_bytes=1024 * 1024),
        cost_estimate=pl.CostEstimate(flops=0, bytes_accessed=2 * moved, transcendentals=0),
    )(*out)
    out = list(out)
    out[6] = pl.pallas_call(
        functools.partial(last_kernel, n_in, rows),
        out_shape=jax.ShapeDtypeStruct(out[6].shape, bf16),
        in_specs=[any_spec] + [vmem_spec] * len(far),
        out_specs=any_spec,
        scratch_shapes=[dma((len(far),))],
        input_output_aliases={0: 0},
        compiler_params=pltpu.CompilerParams(vmem_limit_bytes=1024 * 1024),
    )(out[6], *came)
    return (*out[:6], out[6].reshape(experts, e_rows, width), out[7])


def solution(mesh):
    grouped = P(("gx", "gy"), None)
    in_specs = (P("gx", None, "gy"), P("gx", None, "gy")) + (grouped,) * 6
    out_specs = (grouped,) * 6 + (P("gx", None, "gy"), P(None, "gy"))
    step = functools.partial(local, mesh.shape["gx"], mesh.shape["gy"])
    return jax.shard_map(step, mesh=mesh, in_specs=in_specs, out_specs=out_specs, check_vma=False)
```

```python
import functools
import math

import jax
import jax.numpy as jnp
from jax import lax
from jax.experimental import pallas as pl
from jax.experimental.pallas import tpu as pltpu
from jax.sharding import PartitionSpec as P

MESH = pl.DeviceIdType.MESH

beta_one = 0.9
beta_two = 0.95
learn_rate = 0.01
weight_decay = 0.1
adam_eps = 1e-08
bias_one = 1.0 - 0.9**20
bias_two = 1.0 - 0.95**20


def adam_update(gradient, master, moment, second, clip_factor):
    scaled = clip_factor * gradient
    moment_new = beta_one * moment + (1.0 - beta_one) * scaled
    second_new = beta_two * second + (1.0 - beta_two) * scaled * scaled
    update = moment_new / bias_one / (jnp.sqrt(second_new / bias_two) + adam_eps)
    master_new = master - learn_rate * (update + weight_decay * master)
    return (master_new, moment_new, second_new)


def partner_to(me, k, n):
    if n & (n - 1):
        return lax.rem(me + k, n)
    out, bit = me, 1
    while bit < n:
        if k & bit:
            out = out + bit * (1 - 2 * lax.rem(me // bit, 2))
        bit *= 2
    return out


def partner_from(me, k, n):
    if n & (n - 1):
        return lax.rem(me + n - k, n)
    return partner_to(me, k, n)


def send_order(n):
    return list(range(n - 1, 0, -1))


def col_chunk(width):
    return 256 if width % 256 == 0 else 128


def row_chunk(rows):
    return math.gcd(rows, 16)


def partner_of(me, k, n):
    return (me + k) % n if n & (n - 1) else me ^ k


def far_blocks(n):
    return [n - 2]


def late_rows(rows):
    return math.gcd(rows // 4, 32)


def kept_rows(rows):
    return max(rows * 6 // 8 // 16 * 16, 16) if rows > 16 else rows // 2


top = 2.0**15.5
floor = 2.0**-15.5


def encode(x):
    square = x * x
    fourth = square * square
    eighth = jnp.where(jnp.abs(x) < floor, 0.0, fourth * fourth)
    return jnp.where(x < 0.0, -eighth, eighth)


def decode(y):
    root = jnp.sqrt(jnp.sqrt(jnp.sqrt(jnp.abs(y))))
    return jnp.where(y < 0.0, -root, root)


def step_kernel(
    n_out, n_in, numel,
    eg, ag, em, eo, es, am, ao, as_,
    em_o, eo_o, es_o, am_o, ao_o, as_o, ew_o, aw_o, left,
    mine, held, arep, asum, acode, agot, part, acc,
    ready, late_sem, own_sem, load_sem, state_sem, f_send, f_recv, g_send, g_recv, h_send, h_recv,
    p_send, p_recv, q_send, q_recv, r_send, r_recv, s_send, s_recv, t_send, t_recv,
):
    out_me = lax.axis_index("gx")
    in_me = lax.axis_index("gy")
    rows, width = held.shape[1], held.shape[2]
    block_rows, a_width = arep.shape[1], arep.shape[2]
    a_rows = agot.shape[1]

    def to_in(k):
        return (out_me, partner_to(in_me, k, n_in))

    def to_out(k):
        return (partner_to(out_me, k, n_out), in_me)

    def remote(src, dst, send, recv, where):
        return pltpu.make_async_remote_copy(
            src_ref=src, dst_ref=dst, send_sem=send, recv_sem=recv,
            device_id=where, device_id_type=MESH,
        )

    def rows_at(ref, index, count):
        return ref.at[pl.ds(pl.multiple_of(index * count, count), count)]

    barrier = pltpu.get_barrier_semaphore()

    def signal(sem, where):
        pl.semaphore_signal(sem, inc=1, device_id=where, device_id_type=MESH)

    quarter = n_in // 4
    staged = quarter > 0 and not n_in & (n_in - 1)
    middle = outer = None
    if staged:
        middle = lax.rem(in_me // quarter, 2) != in_me // (2 * quarter)
        outer = jnp.logical_not(middle)
        for k in range(3 * quarter, n_in):
            signal(barrier, to_in(k))

        @pl.when(middle)
        def _():
            for k in range(quarter, 3 * quarter):
                signal(barrier, to_in(k))

        @pl.when(outer)
        def _():
            for k in range(1, quarter):
                signal(barrier, to_in(k))
            for k in range(1, n_out):
                signal(barrier, to_out(k))
    else:
        for k in range(1, n_in):
            signal(barrier, to_in(k))
        for k in range(1, n_out):
            signal(barrier, to_out(k))

    order = send_order(n_in)
    far, near = order[: n_in // 2], order[n_in // 2 :]
    first = far[: n_in // 4] + near[:1]
    rest = near[1:] + far[n_in // 4 :]
    arrival = first + near[1:] + [0] + far[n_in // 4 :]

    def block_of(ref, k):
        return rows_at(ref, partner_to(in_me, k, n_in), rows)

    load = {}
    for k in first + rest + [0]:
        load[k] = pltpu.make_async_copy(block_of(eg, k), block_of(mine, k), load_sem.at[k])
        load[k].start()
    load_rep = pltpu.make_async_copy(rows_at(ag, out_me, block_rows), arep.at[0], own_sem.at[1])
    load_rep.start()
    everyone = n_in - 1 + n_out - 1
    if staged:
        @pl.when(middle)
        def _():
            pl.semaphore_wait(barrier, quarter)

        @pl.when(outer)
        def _():
            pl.semaphore_wait(barrier, everyone)
    else:
        pl.semaphore_wait(barrier, everyone)

    fwd = {}

    def send_fwd(k):
        c = remote(block_of(mine, k), held.at[k], f_send.at[k], f_recv.at[k], to_in(k))
        c.start()
        fwd[k] = c

    for k in far[:quarter]:
        load[k].wait()
        send_fwd(k)
    if staged:
        @pl.when(outer)
        def _():
            for k in range(1, n_out):
                signal(ready, to_out(k))
            if n_out > 1:
                pl.semaphore_wait(ready, n_out - 1)
            signal(ready, to_in(quarter))

        @pl.when(middle)
        def _():
            pl.semaphore_wait(ready, 1)

    rep_copies = {}
    for k in send_order(n_out):
        c = remote(
            rows_at(ag, partner_to(out_me, k, n_out), block_rows), arep.at[k],
            g_send.at[k], g_recv.at[k], to_out(k),
        )
        c.start()
        rep_copies[k] = c
    for k in near[:1]:
        load[k].wait()
        send_fwd(k)

    state = []
    for i, (src, dst) in enumerate(
        ((em, em_o), (eo, eo_o), (es, es_o), (am, am_o), (ao, ao_o), (as_, as_o))
    ):
        c = pltpu.make_async_copy(src, dst, state_sem.at[i])
        c.start()
        state.append(c)

    for k in rest + [0]:
        load[k].wait()
    chunk = col_chunk(width)
    rc = row_chunk(mine.shape[0])

    def square_rows(i, carry):
        r = pl.ds(pl.multiple_of(i * rc, rc), rc)
        for c in range(width // chunk):
            x = mine[r, c * chunk : (c + 1) * chunk].astype(jnp.float32)
            carry = carry + x * x
        return carry

    e_sq = lax.fori_loop(0, mine.shape[0] // rc, square_rows, jnp.zeros((rc, chunk), jnp.float32))

    load_rep.wait()
    for k in send_order(n_out):
        rep_copies[k].wait_recv()
    a_chunk = col_chunk(a_width)
    arc = row_chunk(block_rows)

    def sum_rows(i, carry):
        squares, largest = carry
        r = pl.ds(pl.multiple_of(i * arc, arc), arc)
        for c in range(a_width // a_chunk):
            cols = slice(c * a_chunk, (c + 1) * a_chunk)
            x = arep[0, r, cols].astype(jnp.float32)
            for k in range(1, n_out):
                x = x + arep[k, r, cols].astype(jnp.float32)
            asum[r, cols] = x
            squares = squares + x * x
            largest = jnp.maximum(largest, jnp.abs(x))
        return squares, largest

    zeros = jnp.zeros((arc, a_chunk), jnp.float32)
    a_sq, a_max = lax.fori_loop(0, block_rows // arc, sum_rows, (zeros, zeros))
    total = jnp.sum(e_sq) + jnp.sum(a_sq)
    part[0] = jnp.full(part.shape[1:], total, jnp.float32)

    sq_out = []
    for k in send_order(n_out):
        c = remote(part.at[0], part.at[k], p_send.at[k], p_recv.at[k], to_out(k))
        c.start()
        sq_out.append(c)
    largest = jnp.maximum(jnp.max(a_max), 1e-30)
    scale = jnp.full((1, 1), top, jnp.float32) / largest

    def code_rows(i, _):
        r = pl.ds(pl.multiple_of(i * arc, arc), arc)
        for c in range(a_width // a_chunk):
            cols = slice(c * a_chunk, (c + 1) * a_chunk)
            acode[r, cols] = encode(asum[r, cols] * scale).astype(jnp.bfloat16)
        return 0

    lax.fori_loop(0, block_rows // arc, code_rows, 0)
    own_rows = pltpu.make_async_copy(rows_at(acode, in_me, a_rows), agot.at[0], own_sem.at[2])
    own_rows.start()
    own_grad = pltpu.make_async_copy(rows_at(mine, in_me, rows), held.at[0], own_sem.at[3])
    own_grad.start()
    for c in sq_out:
        c.wait()
    total = jnp.sum(part[:n_out, 0:1, 0:1])
    acc[0, 0:4] = jnp.full((4, acc.shape[2]), total, jnp.float32)
    acc[0, 4:8] = jnp.full((4, acc.shape[2]), largest, jnp.float32)
    sq_in = []
    for k in order:
        c = remote(acc.at[0], acc.at[k], q_send.at[k], q_recv.at[k], to_in(k))
        c.start()
        sq_in.append(c)
    attn_fwd = {}
    for k in order:
        c = remote(
            rows_at(acode, partner_to(in_me, k, n_in), a_rows), agot.at[k],
            h_send.at[k], h_recv.at[k], to_in(k),
        )
        c.start()
        attn_fwd[k] = c
    for k in rest:
        send_fwd(k)
    for c in sq_in:
        c.wait()
    total = jnp.sum(acc[:n_in, 0:1, 0:1])
    clip = 1.0 / jnp.sqrt(jnp.full((1, 1), total, jnp.float32) / numel + 1e-06)

    own_rows.wait()
    for c in state:
        c.wait()
    arow = row_chunk(a_rows)

    def update(k, source, held, factor, load, refs, n_rows, n_cols, cc, rchunk):
        master, moment, second = refs

        def body(i, _):
            r = pl.ds(pl.multiple_of(i * rchunk, rchunk), rchunk)
            for c in range(n_cols // cc):
                cols = pl.ds(pl.multiple_of(source * n_cols + c * cc, 128), cc)
                here = slice(c * cc, (c + 1) * cc)
                g = load(held[k, r, here].astype(jnp.float32))
                a, b, d = adam_update(g, master[r, cols], moment[r, cols], second[r, cols], factor)
                master[r, cols] = a
                moment[r, cols] = b
                second[r, cols] = d
                held[k, r, here] = a.astype(jnp.bfloat16)
            return 0

        lax.fori_loop(0, n_rows // rchunk, body, 0)

    block_base = out_me * block_rows

    def attn_place(owner):
        return aw_o.at[pl.ds(pl.multiple_of(block_base + owner * a_rows, a_rows), a_rows)]

    attn_back = []
    attn_refs = (am_o, ao_o, as_o)
    for k in order + [0]:
        if k:
            attn_fwd[k].wait_recv()
        factor = clip * (acc[k, 4:5, 0:1] / top)
        update(
            k, partner_from(in_me, k, n_in), agot, factor, decode, attn_refs,
            a_rows, a_width, a_chunk, arow,
        )
    for k in order:
        where = (out_me, partner_from(in_me, k, n_in))
        c = remote(agot.at[k], attn_place(in_me), r_send.at[k], r_recv.at[k], where)
        c.start()
        attn_back.append(c)
    attn_own = pltpu.make_async_copy(agot.at[0], attn_place(in_me), own_sem.at[4])
    attn_own.start()

    erow = row_chunk(rows)
    e_refs = (em_o, eo_o, es_o)
    back = []
    gather = []
    for k in arrival:
        if k:
            fwd[k].wait_recv()
        else:
            own_grad.wait()
        update(
            k, partner_from(in_me, k, n_in), held, clip, lambda g: g, e_refs,
            rows, width, chunk, erow,
        )
        if k:
            where = (out_me, partner_from(in_me, k, n_in))
            sent = rows
            if k in far_blocks(n_in):
                sent = rows - kept_rows(rows)
                left[far_blocks(n_in).index(k)] = held[k, sent:rows]
            elif k == n_in - 1:
                sent = rows - late_rows(rows)
                place = pl.ds(pl.multiple_of(in_me * rows + sent, math.gcd(rows, sent)), rows - sent)
                late = remote(
                    held.at[k, sent:rows], ew_o.at[place], late_sem.at[0], late_sem.at[1], where
                )
            place = pl.ds(pl.multiple_of(in_me * rows, rows), sent)
            c = remote(held.at[k, 0:sent], ew_o.at[place], s_send.at[k], s_recv.at[k], where)
            if k not in far_blocks(n_in):
                c.start()
            back.append(c)
        else:
            own_weight = pltpu.make_async_copy(held.at[0], rows_at(ew_o, in_me, rows), own_sem.at[5])
            own_weight.start()
    for k, c in zip([k for k in arrival if k], back):
        if k in far_blocks(n_in):
            c.start()
    late.start()
    back.append(late)
    attn_own.wait()
    for c in attn_back:
        c.wait_recv()
    for k in send_order(n_out):
        mine_rows = rows_at(aw_o, out_me, block_rows)
        c = remote(mine_rows, mine_rows, t_send.at[k], t_recv.at[k], to_out(k))
        c.start()
        gather.append(c)

    for k in order:
        fwd[k].wait_send()
        attn_fwd[k].wait_send()
    for k in send_order(n_out):
        rep_copies[k].wait_send()
    for c in attn_back:
        c.wait_send()
    own_weight.wait()
    for c in gather:
        c.wait()
    for c in back:
        c.wait()


def put_kernel(*refs):
    count = (len(refs) - 1) // 2
    sem = refs[-1]
    copies = [
        pltpu.make_async_copy(refs[i], refs[count + i], sem.at[i]) for i in range(count)
    ]
    for c in copies:
        c.start()
    for c in copies:
        c.wait()


def last_kernel(n_in, rows, *refs):
    count = len(refs) - 3
    out, sem = refs[-2:]
    in_me = lax.axis_index("gy")
    copies = []
    for i, k in enumerate(far_blocks(n_in)):
        keep = refs[1 + i].shape[0]
        start = partner_to(in_me, k, n_in) * rows + (rows - keep)
        place = pl.ds(pl.multiple_of(start, math.gcd(rows, keep)), keep)
        copies.append(pltpu.make_async_copy(refs[1 + i], out.at[place], sem.at[i]))
    for c in copies:
        c.start()
    for c in copies:
        c.wait()


def local(n_out, n_in, eg, ag, em, eo, es, am, ao, as_):
    experts, e_rows, width = eg.shape
    eg = eg.reshape(experts * e_rows, width)
    ag = ag.reshape(ag.shape[1], ag.shape[2])
    numel = (em.shape[0] * em.shape[1] + am.shape[0] * am.shape[1]) * n_out * n_in
    rows = em.shape[0]
    a_rows = am.shape[0]
    a_width = ag.shape[1]
    block_rows = ag.shape[0] // n_out
    f32, bf16 = jnp.float32, jnp.bfloat16
    shapes = [(em.shape, f32)] * 3 + [(am.shape, f32)] * 3 + [(eg.shape, bf16), (ag.shape, bf16)]
    far = far_blocks(n_in)
    shapes += [((len(far), kept_rows(rows), width), bf16)]
    any_spec = pl.BlockSpec(memory_space=pl.ANY)
    vmem_spec = pl.BlockSpec(memory_space=pltpu.VMEM)
    dma = pltpu.SemaphoreType.DMA
    out = pl.pallas_call(
        functools.partial(step_kernel, n_out, n_in, float(numel)),
        out_shape=[pltpu.VMEM(s, d) for s, d in shapes],
        in_specs=[pl.BlockSpec(memory_space=pltpu.HBM)] * 8,
        out_specs=[vmem_spec] * 9,
        scratch_shapes=[
            pltpu.VMEM(eg.shape, bf16),
            pltpu.VMEM((n_in, rows, width), bf16),
            pltpu.VMEM((n_out, block_rows, a_width), bf16),
            pltpu.VMEM((block_rows, a_width), f32),
            pltpu.VMEM((block_rows, a_width), bf16),
            pltpu.VMEM((n_in, a_rows, a_width), bf16),
            pltpu.VMEM((n_out, 8, 128), f32),
            pltpu.VMEM((n_in, 8, 128), f32),
            pltpu.SemaphoreType.REGULAR, dma((2,)),
            dma((6,)), dma((n_in,)), dma((6,)),
            dma((n_in,)), dma((n_in,)),
            dma((n_out,)), dma((n_out,)),
            dma((n_in,)), dma((n_in,)),
            dma((n_out,)), dma((n_out,)),
            dma((n_in,)), dma((n_in,)),
            dma((n_in,)), dma((n_in,)),
            dma((n_in,)), dma((n_in,)),
            dma((n_out,)), dma((n_out,)),
        ],
        compiler_params=pltpu.CompilerParams(
            collective_id=0, has_side_effects=True, vmem_limit_bytes=26 * 1024 * 1024
        ),
    )(eg, ag, em, eo, es, am, ao, as_)
    *out, left = out
    came = [
        lax.ppermute(left[i], "gy", [(j, partner_of(j, k, n_in)) for j in range(n_in)])
        for i, k in enumerate(far)
    ]
    moved = sum(x.size * x.dtype.itemsize for x in out)
    out = pl.pallas_call(
        put_kernel,
        out_shape=[jax.ShapeDtypeStruct(x.shape, x.dtype) for x in out],
        in_specs=[vmem_spec] * 8,
        out_specs=[any_spec] * 8,
        scratch_shapes=[dma((8,))],
        compiler_params=pltpu.CompilerParams(vmem_limit_bytes=1024 * 1024),
        cost_estimate=pl.CostEstimate(flops=0, bytes_accessed=2 * moved, transcendentals=0),
    )(*out)
    out = list(out)
    out[6] = pl.pallas_call(
        functools.partial(last_kernel, n_in, rows),
        out_shape=jax.ShapeDtypeStruct(out[6].shape, bf16),
        in_specs=[any_spec] + [vmem_spec] * len(far),
        out_specs=any_spec,
        scratch_shapes=[dma((len(far),))],
        input_output_aliases={0: 0},
        compiler_params=pltpu.CompilerParams(vmem_limit_bytes=1024 * 1024),
    )(out[6], *came)
    return (*out[:6], out[6].reshape(experts, e_rows, width), out[7])


def solution(mesh):
    grouped = P(("gx", "gy"), None)
    in_specs = (P("gx", None, "gy"), P("gx", None, "gy")) + (grouped,) * 6
    out_specs = (grouped,) * 6 + (P("gx", None, "gy"), P(None, "gy"))
    step = functools.partial(local, mesh.shape["gx"], mesh.shape["gy"])
    return jax.shard_map(step, mesh=mesh, in_specs=in_specs, out_specs=out_specs, check_vma=False)
```
